256 devices in a mesh: row: 8 (over z), col: 32 (over x, y, core).
Axes of the slice: x: 4, y: 4, z: 8, core: 2. Of those that a mesh axis runs over, the one named last changes fastest.
Arguments:
- rho_real: float32 [4096, 4096], P('row', 'col'), may hold values from -2.5 to 4, as said below
- rho_imag: float32 [4096, 4096], P('row', 'col'), may hold values from -2.5 to 2.5, as said below
- hamiltonian: bfloat16 [4096, 4096], P('row', 'col'), may hold values from -1 to 1
- amplitudes: float32 [8, 4096], replicated, may hold values from 0.15 to 0.6
- offsets: int32 [8], replicated, may hold values from -16 to 16
- active_jumps: int32 [1], replicated, may hold values from 4 to 8
Outputs:
- rho_next_real: float32 [4096, 4096], P('row', 'col')
- rho_next_imag: float32 [4096, 4096], P('row', 'col')
The draws below stay inside these ranges and needn't reach their ends.
Inputs may be any that keep to these rules, and one draw needn't show every extreme that they name: `rho_real`: symmetric, with every diagonal entry 0.5 or more. `rho_imag`: antisymmetric.
All inputs are finite; a program needn't handle non-finite values.
Results may differ from the reference program's by a relative error of at most 0.001.
Values may be sent and summed in bfloat16 or wider, within the bound.
A program may use at most 64 MiB of HBM per device.

```python
import math
import jax
import jax.numpy as jnp
from jax import lax

N = 4096
K = 8
OMAX = 16


def fluctuation(key):
    return jnp.clip(jax.random.normal(key, (N, N), jnp.float32), -3.0, 3.0)


def draw_rho_real(key, part):
    values = fluctuation(jax.random.fold_in(key, 11))
    spread = (values + values.T) * 0.35
    diagonal = jax.random.uniform(jax.random.fold_in(key, 12), (N,), jnp.float32, 0.5, 2.0)
    row_index = lax.broadcasted_iota(jnp.int32, (N, N), 0)
    col_index = lax.broadcasted_iota(jnp.int32, (N, N), 1)
    return jnp.where(row_index == col_index, diagonal[:, None], spread)


def draw_rho_imag(key, part):
    values = fluctuation(jax.random.fold_in(key, 21))
    return (values - values.T) * 0.35


def draw_hamiltonian(key, part):
    values = fluctuation(jax.random.fold_in(key, 31))
    return ((values + values.T) * (0.7 / math.sqrt(N))).astype(jnp.bfloat16)


def plant(drawn, own_key, low, high):
    longest = drawn.shape.index(max(drawn.shape))
    spots = []
    for shift in (0, 1):
        where = [jax.random.randint(jax.random.fold_in(own_key, axis), (), 0, length) for axis, length in enumerate(drawn.shape)]
        where[longest] = (where[longest] + shift) % drawn.shape[longest]
        spots.append(tuple(where))
    return drawn.at[spots[0]].set(low).at[spots[1]].set(high)


def setup_inputs(seed: int = 0) -> dict:
    keys = jax.random.split(jax.random.key(seed), 7)
    rho_real = draw_rho_real(jax.random.fold_in(keys[6], 71), 0)
    rho_imag = draw_rho_imag(jax.random.fold_in(keys[6], 71), 0)
    hamiltonian = draw_hamiltonian(jax.random.fold_in(keys[6], 71), 0)
    amplitudes = jnp.clip(jnp.exp(jax.random.uniform(keys[3], (K, N), jnp.float32, math.log(0.15), math.log(0.6))), 0.15, 0.6)
    offsets = plant(jax.random.randint(keys[4], (K,), -OMAX, OMAX + 1), jax.random.fold_in(keys[4], 1), -OMAX, OMAX).astype(jnp.int32)
    active_jumps = jax.random.randint(keys[5], (1,), K // 2, K + 1).astype(jnp.int32)
    return dict(rho_real=rho_real, rho_imag=rho_imag, hamiltonian=hamiltonian, amplitudes=amplitudes, offsets=offsets, active_jumps=active_jumps)


step_size = 0.25


def dissipate(matrix, padded, amplitudes, offsets, active, row_first, col_first):
    height = matrix.shape[1]
    breadth = matrix.shape[2]
    levels = amplitudes.shape[1]
    margin = (padded.shape[1] - height) // 2
    positions = jnp.arange(levels, dtype=jnp.int32)
    summed = jnp.zeros(matrix.shape, matrix.dtype)
    for jump_slot in range(amplitudes.shape[0]):
        offset = offsets[jump_slot].astype(jnp.int32)
        inside = (positions + offset >= 0) & (positions + offset < levels)
        strength = jnp.where(inside, amplitudes[jump_slot], 0.0)
        outflow = jnp.pad(strength * strength, (margin, margin))
        outflow = lax.dynamic_slice_in_dim(outflow, (margin - offset).astype(jnp.int32), levels)
        row_strength = lax.dynamic_slice_in_dim(strength, row_first, height)
        col_strength = lax.dynamic_slice_in_dim(strength, col_first, breadth)
        row_outflow = lax.dynamic_slice_in_dim(outflow, row_first, height)
        col_outflow = lax.dynamic_slice_in_dim(outflow, col_first, breadth)
        corner = (margin + offset).astype(jnp.int32)
        shifted = lax.dynamic_slice(padded, (jnp.int32(0), corner, corner), (2, height, breadth))
        contribution = (row_strength[:, None] * col_strength[None, :]) * shifted - 0.5 * (row_outflow[:, None] + col_outflow[None, :]) * matrix
        summed = summed + jnp.where(jump_slot < active, contribution, 0.0)
    return summed


def drift(real_part, imag_part, hamiltonian, amplitudes, offsets, active):
    real_low = real_part.astype(jnp.bfloat16)
    imag_low = imag_part.astype(jnp.bfloat16)
    left_real = jnp.dot(hamiltonian, real_low, preferred_element_type=jnp.float32)
    right_real = jnp.dot(real_low, hamiltonian, preferred_element_type=jnp.float32)
    left_imag = jnp.dot(hamiltonian, imag_low, preferred_element_type=jnp.float32)
    right_imag = jnp.dot(imag_low, hamiltonian, preferred_element_type=jnp.float32)
    matrix = jnp.stack([real_part, imag_part])
    padded = jnp.pad(matrix, ((0, 0), (OMAX, OMAX), (OMAX, OMAX)))
    loss = dissipate(matrix, padded, amplitudes, offsets, active, jnp.int32(0), jnp.int32(0))
    return left_imag - right_imag + loss[0], right_real - left_real + loss[1]


def reference(rho_real, rho_imag, hamiltonian, amplitudes, offsets, active_jumps):
    active = active_jumps[0]
    first_real, first_imag = drift(rho_real, rho_imag, hamiltonian, amplitudes, offsets, active)
    middle_real = rho_real + step_size * first_real
    middle_imag = rho_imag + step_size * first_imag
    middle_trace = jnp.trace(middle_real)
    rescale = N / middle_trace
    middle_real = middle_real * rescale
    middle_imag = middle_imag * rescale
    second_real, second_imag = drift(middle_real, middle_imag, hamiltonian, amplitudes, offsets, active)
    updated_real = rho_real + 0.5 * step_size * (first_real + second_real)
    updated_imag = rho_imag + 0.5 * step_size * (first_imag + second_imag)
    final_trace = jnp.trace(updated_real)
    rescale = N / final_trace
    return updated_real * rescale, updated_imag * rescale
```

```python
import functools

import jax
import jax.numpy as jnp
from jax import lax
from jax.experimental import pallas as pl
from jax.experimental.pallas import tpu as pltpu
from jax.sharding import Mesh
from jax.sharding import PartitionSpec as P

MESH = pl.DeviceIdType.MESH
STEP = 0.25
OMAX = 16
F32 = jnp.float32
BF16 = jnp.bfloat16
NZ, NX, NY, NC = 8, 4, 4, 2
HEIGHT, WIDTH, SLOTS, LEVELS = 512, 128, 8, 4096
BLOCKS = LEVELS // WIDTH
FIRST = (0, 256)
HALF = 128


def iota(shape, dim):
    return lax.broadcasted_iota(jnp.int32, shape, dim)


class Sends:
    def __init__(self, sems):
        self.sems = sems
        self.made = []

    def __call__(self, src, dst, arrived, **device):
        copy = pltpu.make_async_remote_copy(
            src_ref=src,
            dst_ref=dst,
            send_sem=self.sems.at[len(self.made)],
            recv_sem=arrived,
            device_id=device,
            device_id_type=MESH,
        )
        self.made.append(copy)
        copy.start()

    def drain(self):
        for copy in self.made:
            copy.wait_send()


def wait_for(ref, sem):
    pltpu.make_async_copy(ref, ref, sem).wait()


def kernel(
    real, imag, ham, amp, offsets, active, out_real, out_imag,
    row1, row2, col1, col2, part1, part2, acc, peer,
    traces, hs, hr, xe, shifted, onehot, coef, drift1, middle, diss, ts, tx,
    sent, rows1_in, rows2_in, cols1_in, cols2_in, part_in, peer_in, trace_in, halo_in, turn_in,
):
    z, x, y, c = (lax.axis_index(a) for a in ("z", "x", "y", "c"))
    cb = x * 8 + y * 2 + c
    send = Sends(sent)
    other = 1 - c
    near = {
        ("z", 1): lax.rem(z + 1, NZ), ("z", -1): lax.rem(z + NZ - 1, NZ),
        ("x", 1): lax.rem(x + 1, NX), ("x", -1): lax.rem(x + NX - 1, NX),
        ("y", 1): lax.rem(y + 1, NY), ("y", -1): lax.rem(y + NY - 1, NY),
    }

    def quarter(ref, q):
        return ref[pl.ds(pl.multiple_of(q * WIDTH, WIDTH), WIDTH), :]

    class Gather:
        def __init__(self, row, row_in, col, col_in, part, part_sem):
            self.row, self.row_in, self.col, self.col_in = row, row_in, col, col_in
            self.part, self.part_sem = part, part_sem

        def block(self, p, du, dv, h=None):
            dx, dy = (du, dv) if p == 0 else (dv, du)
            if h is None:
                return self.row.at[dx, dy, :, pl.ds(FIRST[p], 2 * HALF), :]
            return self.row.at[dx, dy, :, pl.ds(FIRST[p] + h * HALF, HALF), :]

        def put(self, p, here, there, axis, sign, h=None):
            send(
                self.block(p, *here, h), self.block(p, *there, h),
                self.row_in.at[p, there[0], there[1], h or 0],
                **{axis: near[axis, sign]},
            )

        def arrived(self, p, du, dv, h=None):
            wait_for(self.block(p, du, dv, h), self.row_in.at[p, du, dv, h or 0])

        def along_u(self, p, du, sign, h=None):
            self.put(p, (du, 0), ((du + sign) % 4, 0), "xy"[p], sign, h)

        def along_v(self, p, du, dv, sign, h=None):
            self.put(p, (du, dv), (du, (dv + sign) % 4), "yx"[p], sign, h)

        def source(self, sign, d):
            return lax.rem(z + NZ - sign * d, NZ)

        def piece(self, owner, j):
            return self.col.at[owner, c if j == 0 else other]

        def along_z(self, sign, d, j):
            piece = self.piece(self.source(sign, d), j)
            send(piece, piece, self.col_in.at[(1 - sign) // 2, d, j], z=near["z", sign])

        def arrived_z(self, sign, d, j):
            wait_for(
                self.piece(self.source(sign, d), j), self.col_in.at[(1 - sign) // 2, d - 1, j]
            )
            if d < 3 or (d == 3 and (j == 0) == (sign == 1)):
                self.along_z(sign, d, j)

        def begin(self):
            send(self.part, self.col.at[z, c], self.part_sem, c=other)
            for p in (0, 1):
                for sign in (1, -1):
                    self.along_u(p, 0, sign)
            for sign in (1, -1):
                self.along_z(sign, 0, 0)
            for p in (0, 1):
                for sign in (1, -1):
                    self.along_v(p, 0, 0, sign)
            wait_for(self.col.at[z, other], self.part_sem)
            for sign in (1, -1):
                self.along_z(sign, 0, 1)

        def step_one(self):
            for p in (0, 1):
                for du, sign in ((1, 1), (3, -1)):
                    self.arrived(p, du, 0)
                    self.along_u(p, du, sign, 0 if sign == 1 else 1)
                    for way in (1, -1):
                        self.along_v(p, du, 0, way)
            for j in (0, 1):
                for sign in (1, -1):
                    self.arrived_z(sign, 1, j)
            for p in (0, 1):
                for sign in (1, -1):
                    self.pass_on(p, 0, sign)

        def pass_on(self, p, du, sign):
            dv = 1 if sign == 1 else 3
            self.arrived(p, du, dv)
            self.along_v(p, du, dv, sign, 0 if sign == 1 else 1)

        def step_two(self):
            for p in (0, 1):
                for h in (0, 1):
                    self.arrived(p, 2, 0, h)
                for way in (1, -1):
                    self.along_v(p, 2, 0, way)
            for j in (0, 1):
                for sign in (1, -1):
                    self.arrived_z(sign, 2, j)
            for du in (1, 3):
                for p in (0, 1):
                    for sign in (1, -1):
                        self.pass_on(p, du, sign)

        def step_three(self):
            for j in (0, 1):
                for sign in (1, -1):
                    self.arrived_z(sign, 3, j)
            for p in (0, 1):
                for sign in (1, -1):
                    self.pass_on(p, 2, sign)

        def finish(self):
            for du in (0, 1, 3, 2):
                for p in (0, 1):
                    for h in (0, 1):
                        self.arrived(p, du, 2, h)
            self.arrived_z(1, 4, 0)
            self.arrived_z(-1, 4, 1)

    def trace_over(step, axis, here, count):
        mine = traces.at[step, here]
        for d in range(1, count):
            send(
                mine, mine, trace_in.at[step, d], **{axis: lax.rem(here + d, count)}
            )

    def trace_total(step, here, count):
        for d in range(1, count):
            wait_for(traces.at[step, lax.rem(here + count - d, count)], trace_in.at[step, d])
        total = traces[step, 0]
        for n in range(1, count):
            total = total + traces[step, n]
        return total

    def halo_begin(stage, state):
        turned = jnp.transpose(state)
        hs[stage, 0] = turned[:OMAX, :].astype(BF16)
        hs[stage, 1] = turned[WIDTH - OMAX :, :].astype(BF16)
        xe[stage, OMAX : OMAX + HEIGHT, 0:WIDTH] = state.astype(BF16)
        hr[stage, 2 * OMAX :, :] = jnp.zeros((WIDTH - 2 * OMAX, HEIGHT), BF16)
        for side, step in ((0, BLOCKS - 1), (1, 1)):
            to = lax.rem(cb + step, BLOCKS)
            send(
                hs.at[stage, side], hr.at[stage, pl.ds(side * OMAX, OMAX), :],
                halo_in.at[stage, side],
                x=to // 8, y=lax.rem(to // 2, NY), c=lax.rem(to, NC),
            )

    def halo_rows(stage):
        for side in (0, 1):
            wait_for(hs.at[stage, side], halo_in.at[stage, side])
        xe[stage, OMAX : OMAX + HEIGHT, WIDTH:] = jnp.transpose(hr[stage].astype(F32)).astype(BF16)
        send(
            xe.at[stage, pl.ds(OMAX, OMAX), :], xe.at[stage, pl.ds(OMAX + HEIGHT, OMAX), :],
            halo_in.at[stage, 2], z=near["z", -1],
        )
        send(
            xe.at[stage, pl.ds(HEIGHT, OMAX), :], xe.at[stage, pl.ds(0, OMAX), :],
            halo_in.at[stage, 3], z=near["z", 1],
        )

    def halo_end(stage):
        for side in (2, 3):
            wait_for(xe.at[stage, pl.ds(0, OMAX), :], halo_in.at[stage, side])

    def coefficients():
        count = active[0]
        slot = iota((SLOTS, WIDTH), 0)
        shift = jnp.zeros((SLOTS, WIDTH), jnp.int32)
        for k in range(SLOTS):
            shift = jnp.where(slot == k, offsets[k], shift)

        def strengths(block):
            at = jnp.minimum(jnp.maximum(block, 0), BLOCKS - 1)
            values = amp[:, pl.ds(pl.multiple_of(at * WIDTH, WIDTH), WIDTH)]
            level = block * WIDTH + iota((SLOTS, WIDTH), 1)
            inside = (level >= 0) & (level < LEVELS) & (level + shift >= 0)
            inside = inside & (level + shift < LEVELS) & (slot < count)
            return jnp.where(inside, values, 0.0)

        blocks = [cb] + [4 * z + r for r in range(4)]
        squares = []
        own = []
        for block in blocks:
            window = [strengths(block + d) for d in (-1, 0, 1)]
            own.append(window[1])
            squares.append(jnp.concatenate([w * w for w in window], axis=1))
        squares = jnp.concatenate(squares + [jnp.zeros_like(squares[0])] * 3, axis=0)
        high = squares.astype(BF16)
        rest = squares - high.astype(F32)
        mid = rest.astype(BF16)
        low = (rest - mid.astype(F32)).astype(BF16)
        parts = jnp.concatenate([high, mid, low], axis=0)
        which = lax.rem(iota(parts.shape, 0), SLOTS)
        total = jnp.zeros((parts.shape[0], WIDTH), F32)
        source = iota((3 * WIDTH, WIDTH), 0)
        target = iota((3 * WIDTH, WIDTH), 1)
        for k in range(SLOTS):
            pick = jnp.where(source == target + (WIDTH - offsets[k]), 1.0, 0.0).astype(BF16)
            chosen = jnp.where(which == k, parts.astype(F32), 0.0).astype(BF16)
            total = total + jnp.dot(chosen, pick, preferred_element_type=F32)
        total = total[0:64] + total[64:128] + total[128:192]
        outflow = [jnp.sum(total[8 * n : 8 * n + 8], axis=0, keepdims=True) for n in range(5)]
        coef[0, 0:SLOTS, :] = own[0]
        coef[0, SLOTS : 2 * SLOTS, :] = jnp.broadcast_to(outflow[0], (SLOTS, WIDTH))
        for r in range(4):
            table = jnp.concatenate(
                [
                    own[1 + r],
                    jnp.broadcast_to(outflow[1 + r], (SLOTS, WIDTH)),
                    jnp.zeros((WIDTH - 2 * SLOTS, WIDTH), F32),
                ],
                axis=0,
            )
            coef[1 + r] = jnp.transpose(table)
        source = iota((2 * WIDTH, WIDTH), 0)
        target = iota((2 * WIDTH, WIDTH), 1)
        for k in range(SLOTS):
            at = target + offsets[k]
            at = jnp.where(at < 0, at + (WIDTH + 2 * OMAX), at)
            onehot[:, k * WIDTH : (k + 1) * WIDTH] = jnp.where(source == at, 1.0, 0.0).astype(BF16)

    def dissipator(stage, state):
        shifted[...] = jnp.dot(xe[stage], onehot[...], preferred_element_type=F32)
        for r in range(4):
            rows = slice(r * WIDTH, (r + 1) * WIDTH)
            by_row = coef[1 + r]
            flow = by_row[:, SLOTS : SLOTS + 1] + coef[0, SLOTS : SLOTS + 1, :]
            total = -0.5 * flow * state[rows, :]
            for k in range(SLOTS):
                span = WIDTH + 2 * OMAX
                moved = shifted[r * WIDTH : r * WIDTH + span, k * WIDTH : (k + 1) * WIDTH]
                moved = pltpu.roll(moved, lax.rem(span - OMAX - offsets[k], span), 0)[0:WIDTH]
                total = total + by_row[:, k : k + 1] * coef[0, k : k + 1, :] * moved
            diss[rows, :] = total

    def commutator(stage):
        def add(n, first):
            dx, dy = n // 4, lax.rem(n, 4)
            xk, yk = lax.rem(x + NX - dx, NX), lax.rem(y + NY - dy, NY)
            owner = 2 * xk + yk // 2
            rows = pl.ds(pl.multiple_of(lax.rem(yk, 2) * WIDTH, WIDTH), WIDTH)
            own = row1[dx, dy, 1] if stage == 0 else row2[dx, dy, 0]
            left = jnp.concatenate([own, row1[dx, dy, 0]], axis=1)
            upper = jnp.concatenate([col1[owner, i, 0, rows, :] for i in range(NC)], axis=1)
            if stage == 0:
                lower = [col1[owner, i, 1, rows, :] for i in range(NC)]
            else:
                lower = [col2[owner, i, 0, rows, :] for i in range(NC)]
            right = jnp.concatenate([upper, jnp.concatenate(lower, axis=1)], axis=0)
            for i in range(NC):
                product = jnp.dot(
                    left, right[:, i * WIDTH : (i + 1) * WIDTH], preferred_element_type=F32
                )
                if first:
                    acc[stage, i] = product
                else:
                    acc[stage, i] += product

        add(jnp.int32(0), True)
        lax.fori_loop(1, 16, lambda n, none: (add(n, False), none)[1], 0)
        send(acc.at[stage, other], peer.at[stage], peer_in.at[stage], c=other)
        wait_for(peer.at[stage], peer_in.at[stage])
        return acc[stage, c] + peer[stage]

    def turn_begin(n, value):
        ts[n] = value.astype(BF16)
        for r in range(4):
            stays = (z == cb // 4) & (r == lax.rem(cb, 4))
            src = ts.at[n, pl.ds(r * WIDTH, WIDTH), :]

            def go(r=r, src=src):
                copy = turn_copy(n, r, src)
                copy.start()

            def keep(r=r):
                tx[n, r] = ts[n, r * WIDTH : (r + 1) * WIDTH, :]

            pl.when(jnp.logical_not(stays))(go)
            pl.when(stays)(keep)

    def turn_copy(n, r, src):
        return pltpu.make_async_remote_copy(
            src_ref=src,
            dst_ref=tx.at[n, lax.rem(cb, 4)],
            send_sem=turn_in.at[n, 0, r],
            recv_sem=turn_in.at[n, 1, lax.rem(cb, 4)],
            device_id=dict(z=cb // 4, x=z // 2, y=2 * lax.rem(z, 2) + r // 2, c=jnp.int32(r % 2)),
            device_id_type=MESH,
        )

    def turn_end(n):
        for r in range(4):
            stays = (z == cb // 4) & (r == lax.rem(cb, 4))

            def done(r=r):
                turn_copy(n, r, ts.at[n, pl.ds(r * WIDTH, WIDTH), :]).wait_send()
                wait_for(tx.at[n, r], turn_in.at[n, 1, r])

            pl.when(jnp.logical_not(stays))(done)

    first = Gather(row1, rows1_in, col1, cols1_in, part1, part_in.at[0])
    row1[0, 0, 0] = ham[...]
    row1[0, 0, 1] = (real[...] + imag[...]).astype(BF16)
    for i in range(2):
        rows = slice(i * WIDTH, (i + 1) * WIDTH)
        part1[0, rows, :] = quarter(ham, 2 * i + other)
        part1[1, rows, :] = -quarter(row1.at[0, 0, 1], 2 * i + other)
        col1[z, c, 0, rows, :] = quarter(ham, 2 * i + c)
        col1[z, c, 1, rows, :] = -quarter(row1.at[0, 0, 1], 2 * i + c)
    on_diagonal = iota((HEIGHT, WIDTH), 0) + z * HEIGHT == iota((HEIGHT, WIDTH), 1) + cb * WIDTH
    diagonal = jnp.sum(jnp.where(on_diagonal, real[...], 0.0), axis=0, keepdims=True)
    diagonal = jnp.sum(diagonal, axis=1, keepdims=True)
    traces[0, z] = jnp.broadcast_to(diagonal, (8, WIDTH))
    trace_over(0, "z", z, NZ)
    first.begin()
    halo_begin(0, real[...] - imag[...])
    first.step_one()
    halo_rows(0)
    traces[1, x] = trace_total(0, z, NZ)
    trace_over(1, "x", x, NX)
    coefficients()
    first.step_two()
    traces[2, y] = trace_total(1, x, NX)
    trace_over(2, "y", y, NY)
    halo_end(0)
    first.step_three()
    dissipator(0, real[...] - imag[...])
    first.finish()
    drift1[...] = diss[...] - commutator(0)
    middle[...] = real[...] - imag[...] + STEP * drift1[...]

    second = Gather(row2, rows2_in, col2, cols2_in, part2, part_in.at[1])
    row2[0, 0, 0] = middle[...].astype(BF16)
    for i in range(2):
        rows = slice(i * WIDTH, (i + 1) * WIDTH)
        part2[0, rows, :] = -quarter(row2.at[0, 0, 0], 2 * i + other)
        col2[z, c, 0, rows, :] = -quarter(row2.at[0, 0, 0], 2 * i + c)
    second.begin()
    halo_begin(1, middle[...])
    traces[3, c] = trace_total(2, y, NY)
    trace_over(3, "c", c, NC)
    second.step_one()
    halo_rows(1)
    rescale = jnp.broadcast_to((LEVELS / trace_total(3, c, NC))[0:1, :], (WIDTH, WIDTH))
    rescale = jnp.concatenate([rescale] * 4, axis=0)
    second.step_two()
    halo_end(1)
    second.step_three()
    dissipator(1, middle[...])
    drift1[...] = drift1[...] + rescale * diss[...]
    turn_begin(0, drift1[...])
    second.finish()
    middle[...] = rescale * commutator(1)
    turn_begin(1, middle[...])
    turn_end(0)
    turn_end(1)
    weight = 0.25 * STEP
    for q in range(4):
        rows = slice(q * WIDTH, (q + 1) * WIDTH)
        scale = rescale[rows, :]
        here_x, here_y = drift1[rows, :], middle[rows, :]
        there_x = jnp.transpose(tx[0, q].astype(F32))
        there_y = jnp.transpose(tx[1, q].astype(F32))
        out_real[rows, :] = scale * (
            real[rows, :] + weight * ((here_x + there_x) + (here_y + there_y))
        )
        out_imag[rows, :] = scale * (
            imag[rows, :] + weight * ((there_x - here_x) + (here_y - there_y))
        )
    send.drain()


def local(real, imag, ham, amp, offsets, active):
    vmem = pl.BlockSpec(memory_space=pltpu.VMEM)
    smem = pl.BlockSpec(memory_space=pltpu.SMEM)
    dma = pltpu.SemaphoreType.DMA
    block = jax.ShapeDtypeStruct((HEIGHT, WIDTH), F32)
    return pl.pallas_call(
        kernel,
        out_shape=(block, block),
        in_specs=[vmem, vmem, vmem, vmem, smem, smem],
        out_specs=(vmem, vmem),
        scratch_shapes=[
            pltpu.VMEM((NX, NY, 2, HEIGHT, WIDTH), BF16),
            pltpu.VMEM((NX, NY, 1, HEIGHT, WIDTH), BF16),
            pltpu.VMEM((NZ, NC, 2, 2 * WIDTH, WIDTH), BF16),
            pltpu.VMEM((NZ, NC, 1, 2 * WIDTH, WIDTH), BF16),
            pltpu.VMEM((2, 2 * WIDTH, WIDTH), BF16),
            pltpu.VMEM((1, 2 * WIDTH, WIDTH), BF16),
            pltpu.VMEM((2, NC, HEIGHT, WIDTH), F32),
            pltpu.VMEM((2, HEIGHT, WIDTH), F32),
            pltpu.VMEM((4, NZ, 8, WIDTH), F32),
            pltpu.VMEM((2, 2, OMAX, HEIGHT), BF16),
            pltpu.VMEM((2, WIDTH, HEIGHT), BF16),
            pltpu.VMEM((2, HEIGHT + 2 * OMAX, 2 * WIDTH), BF16),
            pltpu.VMEM((HEIGHT + 2 * OMAX, SLOTS * WIDTH), F32),
            pltpu.VMEM((2 * WIDTH, SLOTS * WIDTH), BF16),
            pltpu.VMEM((5, WIDTH, WIDTH), F32),
            pltpu.VMEM((HEIGHT, WIDTH), F32),
            pltpu.VMEM((HEIGHT, WIDTH), F32),
            pltpu.VMEM((HEIGHT, WIDTH), F32),
            pltpu.VMEM((2, HEIGHT, WIDTH), BF16),
            pltpu.VMEM((2, 4, WIDTH, WIDTH), BF16),
            dma((144,)),
            dma((2, 4, 4, 2)),
            dma((2, 4, 4, 2)),
            dma((2, 4, 2)),
            dma((2, 4, 2)),
            dma((2,)),
            dma((2,)),
            dma((4, NZ)),
            dma((2, 4)),
            dma((2, 2, 4)),
        ],
        compiler_params=pltpu.CompilerParams(
            has_side_effects=True, vmem_limit_bytes=48 * 1024 * 1024
        ),
    )(real, imag, ham, amp, offsets, active)


def solution(mesh):
    split = Mesh(mesh.devices.reshape(NZ, NX, NY, NC), ("z", "x", "y", "c"))
    tiled = P("z", ("x", "y", "c"))
    return jax.shard_map(
        local,
        mesh=split,
        in_specs=(tiled, tiled, tiled, P(), P(), P()),
        out_specs=(tiled, tiled),
        check_vma=False,
    )
```

```python
import functools

import jax
import jax.numpy as jnp
from jax import lax
from jax.experimental import pallas as pl
from jax.experimental.pallas import tpu as pltpu
from jax.sharding import Mesh
from jax.sharding import PartitionSpec as P

MESH = pl.DeviceIdType.MESH
STEP = 0.25
OMAX = 16
F32 = jnp.float32
BF16 = jnp.bfloat16
NZ, NX, NY, NC = 8, 4, 4, 2
HEIGHT, WIDTH, SLOTS, LEVELS = 512, 128, 8, 4096
BLOCKS = LEVELS // WIDTH
FIRST = (0, 256)
HALF = 128


def iota(shape, dim):
    return lax.broadcasted_iota(jnp.int32, shape, dim)


class Sends:
    def __init__(self, sems):
        self.sems = sems
        self.made = []

    def __call__(self, src, dst, arrived, **device):
        copy = pltpu.make_async_remote_copy(
            src_ref=src,
            dst_ref=dst,
            send_sem=self.sems.at[len(self.made)],
            recv_sem=arrived,
            device_id=device,
            device_id_type=MESH,
        )
        self.made.append(copy)
        copy.start()

    def drain(self):
        for copy in self.made:
            copy.wait_send()


def wait_for(ref, sem):
    pltpu.make_async_copy(ref, ref, sem).wait()


def kernel(
    real_in, imag_in, ham_in, amp_in, offsets_in, active_in, out_real, out_imag,
    real, imag, ham, amp, offsets, active, loaded,
    row1, row2, col1, col2, part1, part2, acc, peer,
    traces, hs, hr, xe, shifted, onehot, coef, drift1, middle, diss, ts, tr, tx,
    sent, rows1_in, rows2_in, cols1_in, cols2_in, part_in, peer_in, trace_in, halo_in, spread_in, turn_in,
):
    z, x, y, c = (lax.axis_index(a) for a in ("z", "x", "y", "c"))
    cb = x * 8 + y * 2 + c
    send = Sends(sent)
    other = 1 - c
    near = {
        ("z", 1): lax.rem(z + 1, NZ), ("z", -1): lax.rem(z + NZ - 1, NZ),
        ("x", 1): lax.rem(x + 1, NX), ("x", -1): lax.rem(x + NX - 1, NX),
        ("y", 1): lax.rem(y + 1, NY), ("y", -1): lax.rem(y + NY - 1, NY),
    }

    loads = [
        pltpu.make_async_copy(src, dst, loaded.at[n])
        for n, (src, dst) in enumerate(
            ((ham_in, ham), (real_in, real), (imag_in, imag), (amp_in, amp),
             (offsets_in, offsets), (active_in, active))
        )
    ]
    for load in loads:
        load.start()
    aside = lax.rem(cb + BLOCKS - 1 + 2 * c, BLOCKS)
    barrier = pltpu.get_barrier_semaphore()
    greeted = [{axis: at} for (axis, _), at in near.items()] + [
        dict(c=other), dict(x=aside // 8, y=lax.rem(aside // 2, NY), c=other)
    ]
    for device in greeted:
        pl.semaphore_signal(barrier, inc=1, device_id=device, device_id_type=MESH)

    def quarter(ref, q):
        return ref[pl.ds(pl.multiple_of(q * WIDTH, WIDTH), WIDTH), :]

    class Gather:
        def __init__(self, row, row_in, col, col_in, part, part_sem):
            self.row, self.row_in, self.col, self.col_in = row, row_in, col, col_in
            self.part, self.part_sem = part, part_sem

        def block(self, p, du, dv, h=None):
            dx, dy = (du, dv) if p == 0 else (dv, du)
            if h is None:
                return self.row.at[dx, dy, :, pl.ds(FIRST[p], 2 * HALF), :]
            return self.row.at[dx, dy, :, pl.ds(FIRST[p] + h * HALF, HALF), :]

        def put(self, p, here, there, axis, sign, h=None):
            send(
                self.block(p, *here, h), self.block(p, *there, h),
                self.row_in.at[p, there[0], there[1], h or 0],
                **{axis: near[axis, sign]},
            )

        def arrived(self, p, du, dv, h=None):
            wait_for(self.block(p, du, dv, h), self.row_in.at[p, du, dv, h or 0])

        def along_u(self, p, du, sign, h=None):
            self.put(p, (du, 0), ((du + sign) % 4, 0), "xy"[p], sign, h)

        def along_v(self, p, du, dv, sign, h=None):
            self.put(p, (du, dv), (du, (dv + sign) % 4), "yx"[p], sign, h)

        def source(self, sign, d):
            return lax.rem(z + NZ - sign * d, NZ)

        def piece(self, owner, j):
            return self.col.at[owner, c if j == 0 else other]

        def along_z(self, sign, d, j):
            piece = self.piece(self.source(sign, d), j)
            send(piece, piece, self.col_in.at[(1 - sign) // 2, d, j], z=near["z", sign])

        def arrived_z(self, sign, d, j):
            wait_for(
                self.piece(self.source(sign, d), j), self.col_in.at[(1 - sign) // 2, d - 1, j]
            )
            if d < 3 or (d == 3 and (j == 0) == (sign == 1)):
                self.along_z(sign, d, j)

        def begin(self):
            send(self.part, self.col.at[z, c], self.part_sem, c=other)
            for p in (0, 1):
                for sign in (1, -1):
                    self.along_u(p, 0, sign)
            for sign in (1, -1):
                self.along_z(sign, 0, 0)
            for p in (0, 1):
                for sign in (1, -1):
                    self.along_v(p, 0, 0, sign)
            wait_for(self.col.at[z, other], self.part_sem)
            for sign in (1, -1):
                self.along_z(sign, 0, 1)

        def step_one(self):
            for p in (0, 1):
                for du, sign in ((1, 1), (3, -1)):
                    self.arrived(p, du, 0)
                    self.along_u(p, du, sign, 0 if sign == 1 else 1)
                    for way in (1, -1):
                        self.along_v(p, du, 0, way)
            for j in (0, 1):
                for sign in (1, -1):
                    self.arrived_z(sign, 1, j)
            for p in (0, 1):
                for sign in (1, -1):
                    self.pass_on(p, 0, sign)

        def pass_on(self, p, du, sign):
            dv = 1 if sign == 1 else 3
            self.arrived(p, du, dv)
            self.along_v(p, du, dv, sign, 0 if sign == 1 else 1)

        def step_two(self):
            for p in (0, 1):
                for h in (0, 1):
                    self.arrived(p, 2, 0, h)
                for way in (1, -1):
                    self.along_v(p, 2, 0, way)
            for j in (0, 1):
                for sign in (1, -1):
                    self.arrived_z(sign, 2, j)
            for du in (1, 3):
                for p in (0, 1):
                    for sign in (1, -1):
                        self.pass_on(p, du, sign)

        def step_three(self):
            for j in (0, 1):
                for sign in (1, -1):
                    self.arrived_z(sign, 3, j)
            for p in (0, 1):
                for sign in (1, -1):
                    self.pass_on(p, 2, sign)

        def finish_z(self):
            self.arrived_z(1, 4, 0)
            self.arrived_z(-1, 4, 1)

        def finish(self):
            for du in (0, 1, 3, 2):
                for p in (0, 1):
                    for h in (0, 1):
                        self.arrived(p, du, 2, h)

    def trace_over(step, axis, here, count):
        mine = traces.at[step, here]
        for d in range(1, count):
            send(
                mine, mine, trace_in.at[step, d], **{axis: lax.rem(here + d, count)}
            )

    def trace_total(step, here, count):
        for d in range(1, count):
            wait_for(traces.at[step, lax.rem(here + count - d, count)], trace_in.at[step, d])
        total = traces[step, 0]
        for n in range(1, count):
            total = total + traces[step, n]
        return total

    def halo_begin(stage, state):
        turned = jnp.transpose(state)
        hs[stage, 0] = turned[:OMAX, :].astype(BF16)
        hs[stage, 1] = turned[WIDTH - OMAX :, :].astype(BF16)
        xe[stage, OMAX : OMAX + HEIGHT, 0:WIDTH] = state.astype(BF16)
        hr[stage, 2 * OMAX :, :] = jnp.zeros((WIDTH - 2 * OMAX, HEIGHT), BF16)
        for side, step in ((0, BLOCKS - 1), (1, 1)):
            to = lax.rem(cb + step, BLOCKS)
            send(
                hs.at[stage, side], hr.at[stage, pl.ds(side * OMAX, OMAX), :],
                halo_in.at[stage, side],
                x=to // 8, y=lax.rem(to // 2, NY), c=lax.rem(to, NC),
            )

    def halo_rows(stage):
        for side in (0, 1):
            wait_for(hs.at[stage, side], halo_in.at[stage, side])
        xe[stage, OMAX : OMAX + HEIGHT, WIDTH:] = jnp.transpose(hr[stage].astype(F32)).astype(BF16)
        send(
            xe.at[stage, pl.ds(OMAX, OMAX), :], xe.at[stage, pl.ds(OMAX + HEIGHT, OMAX), :],
            halo_in.at[stage, 2], z=near["z", -1],
        )
        send(
            xe.at[stage, pl.ds(HEIGHT, OMAX), :], xe.at[stage, pl.ds(0, OMAX), :],
            halo_in.at[stage, 3], z=near["z", 1],
        )

    def halo_end(stage):
        for side in (2, 3):
            wait_for(xe.at[stage, pl.ds(0, OMAX), :], halo_in.at[stage, side])

    def coefficients():
        count = active[0]
        slot = iota((SLOTS, WIDTH), 0)
        shift = jnp.zeros((SLOTS, WIDTH), jnp.int32)
        for k in range(SLOTS):
            shift = jnp.where(slot == k, offsets[k], shift)

        def strengths(block):
            at = jnp.minimum(jnp.maximum(block, 0), BLOCKS - 1)
            values = amp[:, pl.ds(pl.multiple_of(at * WIDTH, WIDTH), WIDTH)]
            level = block * WIDTH + iota((SLOTS, WIDTH), 1)
            inside = (level >= 0) & (level < LEVELS) & (level + shift >= 0)
            inside = inside & (level + shift < LEVELS) & (slot < count)
            return jnp.where(inside, values, 0.0)

        blocks = [cb] + [4 * z + r for r in range(4)]
        squares = []
        own = []
        for block in blocks:
            window = [strengths(block + d) for d in (-1, 0, 1)]
            own.append(window[1])
            squares.append(jnp.concatenate([w * w for w in window], axis=1))
        squares = jnp.concatenate(squares + [jnp.zeros_like(squares[0])] * 3, axis=0)
        high = squares.astype(BF16)
        rest = squares - high.astype(F32)
        mid = rest.astype(BF16)
        low = (rest - mid.astype(F32)).astype(BF16)
        parts = jnp.concatenate([high, mid, low], axis=0)
        which = lax.rem(iota(parts.shape, 0), SLOTS)
        total = jnp.zeros((parts.shape[0], WIDTH), F32)
        source = iota((3 * WIDTH, WIDTH), 0)
        target = iota((3 * WIDTH, WIDTH), 1)
        for k in range(SLOTS):
            pick = jnp.where(source == target + (WIDTH - offsets[k]), 1.0, 0.0).astype(BF16)
            chosen = jnp.where(which == k, parts.astype(F32), 0.0).astype(BF16)
            total = total + jnp.dot(chosen, pick, preferred_element_type=F32)
        total = total[0:64] + total[64:128] + total[128:192]
        outflow = [jnp.sum(total[8 * n : 8 * n + 8], axis=0, keepdims=True) for n in range(5)]
        coef[0, 0:SLOTS, :] = own[0]
        coef[0, SLOTS : 2 * SLOTS, :] = jnp.broadcast_to(outflow[0], (SLOTS, WIDTH))
        for r in range(4):
            table = jnp.concatenate(
                [
                    own[1 + r],
                    jnp.broadcast_to(outflow[1 + r], (SLOTS, WIDTH)),
                    jnp.zeros((WIDTH - 2 * SLOTS, WIDTH), F32),
                ],
                axis=0,
            )
            coef[1 + r] = jnp.transpose(table)
        source = iota((2 * WIDTH, WIDTH), 0)
        target = iota((2 * WIDTH, WIDTH), 1)
        for k in range(SLOTS):
            at = target + offsets[k]
            at = jnp.where(at < 0, at + (WIDTH + 2 * OMAX), at)
            onehot[:, k * WIDTH : (k + 1) * WIDTH] = jnp.where(source == at, 1.0, 0.0).astype(BF16)

    def dissipator(stage, state):
        shifted[...] = jnp.dot(xe[stage], onehot[...], preferred_element_type=F32)
        for r in range(4):
            rows = slice(r * WIDTH, (r + 1) * WIDTH)
            by_row = coef[1 + r]
            flow = by_row[:, SLOTS : SLOTS + 1] + coef[0, SLOTS : SLOTS + 1, :]
            total = -0.5 * flow * state[rows, :]
            for k in range(SLOTS):
                span = WIDTH + 2 * OMAX
                moved = shifted[r * WIDTH : r * WIDTH + span, k * WIDTH : (k + 1) * WIDTH]
                moved = pltpu.roll(moved, lax.rem(span - OMAX - offsets[k], span), 0)[0:WIDTH]
                total = total + by_row[:, k : k + 1] * coef[0, k : k + 1, :] * moved
            diss[rows, :] = total

    def commutator(stage, late):
        lefts, rights = [], []
        for dx in range(NX):
            for dy in range(NY):
                if (dx == 2 or dy == 2 or (dx, dy) == (3, 3)) != late:
                    continue
                xk, yk = lax.rem(x + NX - dx, NX), lax.rem(y + NY - dy, NY)
                owner = 2 * xk + yk // 2
                rows = pl.ds(pl.multiple_of(lax.rem(yk, 2) * WIDTH, WIDTH), WIDTH)
                lefts.append(row1[dx, dy, 1] if stage == 0 else row2[dx, dy, 0])
                lefts.append(row1[dx, dy, 0])
                upper = [col1[owner, i, 0, rows, :] for i in range(NC)]
                if stage == 0:
                    lower = [col1[owner, i, 1, rows, :] for i in range(NC)]
                else:
                    lower = [col2[owner, i, 0, rows, :] for i in range(NC)]
                rights.append(jnp.concatenate(upper, axis=1))
                rights.append(jnp.concatenate(lower, axis=1))
        product = jnp.dot(
            jnp.concatenate(lefts, axis=1),
            jnp.concatenate(rights, axis=0),
            preferred_element_type=F32,
        )
        for i in range(NC):
            mine = product[:, i * WIDTH : (i + 1) * WIDTH]
            if late:
                acc[stage, i] += mine
            else:
                acc[stage, i] = mine

    def joined(stage):
        send(acc.at[stage, other], peer.at[stage], peer_in.at[stage], c=other)
        wait_for(peer.at[stage], peer_in.at[stage])
        return acc[stage, c] + peer[stage]

    def spread_begin(n, value):
        ts[n] = value.astype(BF16)
        for d in range(1, NX):
            to = lax.rem(x + d, NX)
            send(
                ts.at[n, pl.ds(pl.multiple_of(to * WIDTH, WIDTH), WIDTH), :],
                tr.at[n, x], spread_in.at[n, d], x=to,
            )
        tr[n, x] = ts[n, pl.ds(pl.multiple_of(x * WIDTH, WIDTH), WIDTH), :]

    def turn_copy(n, s):
        return pltpu.make_async_remote_copy(
            src_ref=tr.at[n, s],
            dst_ref=tx.at[n, lax.rem(cb, 4)],
            send_sem=turn_in.at[n, 0, s],
            recv_sem=turn_in.at[n, 1, lax.rem(cb, 4)],
            device_id=dict(
                z=2 * s + y // 2, x=z // 2, y=2 * lax.rem(z, 2) + x // 2, c=lax.rem(x, 2)
            ),
            device_id_type=MESH,
        )

    def turn_stays(s):
        there = (2 * s + y // 2 == z) & (z // 2 == x)
        return there & (2 * lax.rem(z, 2) + x // 2 == y) & (lax.rem(x, 2) == c)

    def turn_begin(n):
        for d in range(1, NX):
            wait_for(tr.at[n, lax.rem(x + NX - d, NX)], spread_in.at[n, d])
        for s in range(NX):

            def go(s=s):
                turn_copy(n, s).start()

            def keep(s=s):
                tx[n, lax.rem(cb, 4)] = tr[n, s]

            pl.when(jnp.logical_not(turn_stays(s)))(go)
            pl.when(turn_stays(s))(keep)

    def turn_end(n):
        for s in range(NX):

            def left(s=s):
                turn_copy(n, s).wait_send()

            pl.when(jnp.logical_not(turn_stays(s)))(left)
        for q in range(4):
            own = (cb // 4 == z) & (2 * lax.rem(z, 2) + q // 2 == y) & (q % 2 == c)

            def arrived(q=q):
                wait_for(tx.at[n, q], turn_in.at[n, 1, q])

            own = own & (lax.rem(cb, 4) == x)
            pl.when(jnp.logical_not(own))(arrived)

    first = Gather(row1, rows1_in, col1, cols1_in, part1, part_in.at[0])
    for load in loads[:3]:
        load.wait()
    row1[0, 0, 0] = ham[...]
    row1[0, 0, 1] = (real[...] + imag[...]).astype(BF16)
    for i in range(2):
        rows = slice(i * WIDTH, (i + 1) * WIDTH)
        part1[0, rows, :] = quarter(ham, 2 * i + other)
        part1[1, rows, :] = -quarter(row1.at[0, 0, 1], 2 * i + other)
        col1[z, c, 0, rows, :] = quarter(ham, 2 * i + c)
        col1[z, c, 1, rows, :] = -quarter(row1.at[0, 0, 1], 2 * i + c)
    on_diagonal = iota((HEIGHT, WIDTH), 0) + z * HEIGHT == iota((HEIGHT, WIDTH), 1) + cb * WIDTH
    diagonal = jnp.sum(jnp.where(on_diagonal, real[...], 0.0), axis=0, keepdims=True)
    diagonal = jnp.sum(diagonal, axis=1, keepdims=True)
    traces[0, x] = jnp.broadcast_to(diagonal, (8, WIDTH))
    pl.semaphore_wait(barrier, len(greeted))
    first.begin()
    halo_begin(0, real[...] - imag[...])
    first.step_one()
    halo_rows(0)
    for load in loads[3:]:
        load.wait()
    coefficients()
    first.step_two()
    trace_over(0, "x", x, NX)
    halo_end(0)
    first.step_three()
    traces[1, y] = trace_total(0, x, NX)
    trace_over(1, "y", y, NY)
    dissipator(0, real[...] - imag[...])
    first.finish_z()
    commutator(0, False)
    traces[2, c] = trace_total(1, y, NY)
    trace_over(2, "c", c, NC)
    first.finish()
    commutator(0, True)
    traces[3, z] = trace_total(2, c, NC)
    trace_over(3, "z", z, NZ)
    drift1[...] = diss[...] - joined(0)
    middle[...] = real[...] - imag[...] + STEP * drift1[...]

    second = Gather(row2, rows2_in, col2, cols2_in, part2, part_in.at[1])
    row2[0, 0, 0] = middle[...].astype(BF16)
    for i in range(2):
        rows = slice(i * WIDTH, (i + 1) * WIDTH)
        part2[0, rows, :] = -quarter(row2.at[0, 0, 0], 2 * i + other)
        col2[z, c, 0, rows, :] = -quarter(row2.at[0, 0, 0], 2 * i + c)
    second.begin()
    halo_begin(1, middle[...])
    second.step_one()
    halo_rows(1)
    second.step_two()
    halo_end(1)
    second.step_three()
    dissipator(1, middle[...])
    rescale = jnp.broadcast_to((LEVELS / trace_total(3, z, NZ))[0:1, :], (WIDTH, WIDTH))
    rescale = jnp.concatenate([rescale] * 4, axis=0)
    drift1[...] = drift1[...] + rescale * diss[...]
    spread_begin(0, drift1[...])
    second.finish_z()
    commutator(1, False)
    turn_begin(0)
    second.finish()
    commutator(1, True)
    middle[...] = rescale * joined(1)
    spread_begin(1, middle[...])
    turn_end(0)
    weight = 0.25 * STEP
    turn_begin(1)
    for q in range(4):
        rows = slice(q * WIDTH, (q + 1) * WIDTH)
        there = jnp.transpose(tx[0, q].astype(F32))
        out_real[rows, :] = real[rows, :] + weight * (drift1[rows, :] + there + middle[rows, :])
        out_imag[rows, :] = imag[rows, :] + weight * (there - drift1[rows, :] + middle[rows, :])
    turn_end(1)
    for q in range(4):
        rows = slice(q * WIDTH, (q + 1) * WIDTH)
        there = weight * jnp.transpose(tx[1, q].astype(F32))
        out_real[rows, :] = rescale[rows, :] * (out_real[rows, :] + there)
        out_imag[rows, :] = rescale[rows, :] * (out_imag[rows, :] - there)
    send.drain()


def local(real, imag, ham, amp, offsets, active):
    vmem = pl.BlockSpec(memory_space=pltpu.VMEM)
    hbm = pl.BlockSpec(memory_space=pltpu.HBM)
    dma = pltpu.SemaphoreType.DMA
    block = jax.ShapeDtypeStruct((HEIGHT, WIDTH), F32)
    return pl.pallas_call(
        kernel,
        out_shape=(block, block),
        in_specs=[hbm] * 6,
        out_specs=(vmem, vmem),
        scratch_shapes=[
            pltpu.VMEM((HEIGHT, WIDTH), F32),
            pltpu.VMEM((HEIGHT, WIDTH), F32),
            pltpu.VMEM((HEIGHT, WIDTH), BF16),
            pltpu.VMEM((SLOTS, LEVELS), F32),
            pltpu.SMEM((SLOTS,), jnp.int32),
            pltpu.SMEM((1,), jnp.int32),
            dma((6,)),
            pltpu.VMEM((NX, NY, 2, HEIGHT, WIDTH), BF16),
            pltpu.VMEM((NX, NY, 1, HEIGHT, WIDTH), BF16),
            pltpu.VMEM((NZ, NC, 2, 2 * WIDTH, WIDTH), BF16),
            pltpu.VMEM((NZ, NC, 1, 2 * WIDTH, WIDTH), BF16),
            pltpu.VMEM((2, 2 * WIDTH, WIDTH), BF16),
            pltpu.VMEM((1, 2 * WIDTH, WIDTH), BF16),
            pltpu.VMEM((2, NC, HEIGHT, WIDTH), F32),
            pltpu.VMEM((2, HEIGHT, WIDTH), F32),
            pltpu.VMEM((4, NZ, 8, WIDTH), F32),
            pltpu.VMEM((2, 2, OMAX, HEIGHT), BF16),
            pltpu.VMEM((2, WIDTH, HEIGHT), BF16),
            pltpu.VMEM((2, HEIGHT + 2 * OMAX, 2 * WIDTH), BF16),
            pltpu.VMEM((HEIGHT + 2 * OMAX, SLOTS * WIDTH), F32),
            pltpu.VMEM((2 * WIDTH, SLOTS * WIDTH), BF16),
            pltpu.VMEM((5, WIDTH, WIDTH), F32),
            pltpu.VMEM((HEIGHT, WIDTH), F32),
            pltpu.VMEM((HEIGHT, WIDTH), F32),
            pltpu.VMEM((HEIGHT, WIDTH), F32),
            pltpu.VMEM((2, HEIGHT, WIDTH), BF16),
            pltpu.VMEM((2, 4, WIDTH, WIDTH), BF16),
            pltpu.VMEM((2, 4, WIDTH, WIDTH), BF16),
            dma((152,)),
            dma((2, 4, 4, 2)),
            dma((2, 4, 4, 2)),
            dma((2, 4, 2)),
            dma((2, 4, 2)),
            dma((2,)),
            dma((2,)),
            dma((4, NZ)),
            dma((2, 4)),
            dma((2, 4)),
            dma((2, 2, 4)),
        ],
        compiler_params=pltpu.CompilerParams(
            has_side_effects=True, collective_id=0, vmem_limit_bytes=48 * 1024 * 1024
        ),
    )(real, imag, ham, amp, offsets, active)


def solution(mesh):
    split = Mesh(mesh.devices.reshape(NZ, NX, NY, NC), ("z", "x", "y", "c"))
    tiled = P("z", ("x", "y", "c"))
    return jax.shard_map(
        local,
        mesh=split,
        in_specs=(tiled, tiled, tiled, P(), P(), P()),
        out_specs=(tiled, tiled),
        check_vma=False,
    )
```

```python
import functools

import jax
import jax.numpy as jnp
from jax import lax
from jax.experimental import pallas as pl
from jax.experimental.pallas import tpu as pltpu
from jax.sharding import Mesh
from jax.sharding import PartitionSpec as P

MESH = pl.DeviceIdType.MESH
STEP = 0.25
OMAX = 16
F32 = jnp.float32
BF16 = jnp.bfloat16
NZ, NX, NY, NC = 8, 4, 4, 2
HEIGHT, WIDTH, SLOTS, LEVELS = 512, 128, 8, 4096
BLOCKS = LEVELS // WIDTH
FIRST = (0, 256)
HALF = 128


def iota(shape, dim):
    return lax.broadcasted_iota(jnp.int32, shape, dim)


class Sends:
    def __init__(self, sems):
        self.sems = sems

    def __call__(self, group, src, dst, arrived, **device):
        pltpu.make_async_remote_copy(
            src_ref=src,
            dst_ref=dst,
            send_sem=self.sems.at[group],
            recv_sem=arrived,
            device_id=device,
            device_id_type=MESH,
        ).start()

    def drain(self, *totals):
        for group, ref in enumerate(totals):
            wait_for(ref, self.sems.at[group])


def wait_for(ref, sem):
    pltpu.make_async_copy(ref, ref, sem).wait()


def kernel(
    real_in, imag_in, ham_in, amp_in, offsets_in, active_in, next_real, next_imag, next_factor,
    real, imag, ham, amp, offsets, active, loaded, out_real, out_imag, factor, stored,
    row1, row2, col1, col2, part1, part2, acc, peer,
    traces, hs, hr, xe, shifted, onehot, coef, drift1, middle, diss, ts, tr, tx,
    sent, rows1_in, rows2_in, last_in, cols1_in, cols2_in, part_in, peer_in, trace_in, halo_in, spread_in, turn_in,
):
    z, x, y, c = (lax.axis_index(a) for a in ("z", "x", "y", "c"))
    cb = x * 8 + y * 2 + c
    send = Sends(sent)
    other = 1 - c
    near = {
        ("z", 1): lax.rem(z + 1, NZ), ("z", -1): lax.rem(z + NZ - 1, NZ),
        ("x", 1): lax.rem(x + 1, NX), ("x", -1): lax.rem(x + NX - 1, NX),
        ("y", 1): lax.rem(y + 1, NY), ("y", -1): lax.rem(y + NY - 1, NY),
    }

    loads = [
        pltpu.make_async_copy(src, dst, loaded.at[n])
        for n, (src, dst) in enumerate(
            ((ham_in, ham), (real_in, real), (imag_in, imag), (amp_in, amp),
             (offsets_in, offsets), (active_in, active))
        )
    ]
    for load in loads:
        load.start()
    aside = lax.rem(cb + BLOCKS - 1 + 2 * c, BLOCKS)
    barrier = pltpu.get_barrier_semaphore()
    greeted = [{axis: at} for (axis, _), at in near.items()] + [
        dict(c=other), dict(x=aside // 8, y=lax.rem(aside // 2, NY), c=other)
    ]
    for device in greeted:
        pl.semaphore_signal(barrier, inc=1, device_id=device, device_id_type=MESH)

    def quarter(ref, q):
        return ref[pl.ds(pl.multiple_of(q * WIDTH, WIDTH), WIDTH), :]

    class Gather:
        def __init__(self, group, row, row_in, last_in, col, col_in, part, part_sem):
            self.group, self.row, self.row_in, self.last_in = group, row, row_in, last_in
            self.col, self.col_in, self.part, self.part_sem = col, col_in, part, part_sem
            self.arrays = range(part.shape[0])

        def block(self, p, i, du, dv, h=None):
            slot = 4 * du + dv if p == 0 else 4 * dv + du
            first, count = (0, 2 * HALF) if h is None else (h * HALF, HALF)
            return self.row.at[slot, i, pl.ds(FIRST[p] + first, count), :]

        def arrival(self, p, i, du, dv):
            if dv == 2:
                return self.last_in
            if dv == 0:
                return self.row_in.at[i, p, (None, 0, 2, 1)[du]]
            return self.row_in.at[i, p, (3 if dv == 1 else 7) + du]

        def put(self, p, i, here, there, axis, sign, h=None):
            send(
                self.group, self.block(p, i, *here, h), self.block(p, i, *there, h),
                self.arrival(p, i, *there), **{axis: near[axis, sign]},
            )

        def arrived(self, p, i, du, dv):
            wait_for(self.block(p, i, du, dv), self.arrival(p, i, du, dv))

        def along_u(self, p, i, du, sign, h=None):
            self.put(p, i, (du, 0), ((du + sign) % 4, 0), "xy"[p], sign, h)

        def along_v(self, p, i, du, dv, sign, h=None):
            self.put(p, i, (du, dv), (du, (dv + sign) % 4), "yx"[p], sign, h)

        def piece(self, i, sign, d, j):
            owner = lax.rem(z + NZ - sign * d, NZ)
            return self.col.at[owner * NC + (c if j == 0 else other), i]

        def arrival_z(self, i, sign, d, j):
            return self.col_in.at[i, (1 - sign) // 2, min(2 * (d - 1) + j, 6)]

        def along_z(self, i, sign, d, j):
            piece = self.piece(i, sign, d, j)
            send(
                self.group + 1, piece, piece, self.arrival_z(i, sign, d + 1, j),
                z=near["z", sign],
            )

        def arrived_z(self, i, sign, d, j):
            wait_for(self.piece(i, sign, d, j), self.arrival_z(i, sign, d, j))
            if d < 3 or (d == 3 and (j == 0) == (sign == 1)):
                self.along_z(i, sign, d, j)

        def begin(self):
            here = z * NC
            send(self.group + 1, self.part, self.col.at[here + c], self.part_sem, c=other)
            for i in self.arrays:
                for p in (0, 1):
                    for sign in (1, -1):
                        self.along_u(p, i, 0, sign)
                for sign in (1, -1):
                    self.along_z(i, sign, 0, 0)
            for i in self.arrays:
                for p in (0, 1):
                    for sign in (1, -1):
                        self.along_v(p, i, 0, 0, sign)
            wait_for(self.col.at[here + other], self.part_sem)
            for i in self.arrays:
                for sign in (1, -1):
                    self.along_z(i, sign, 0, 1)

        def step_z(self, d, j):
            for i in self.arrays:
                for sign in (1, -1):
                    self.arrived_z(i, sign, d, j)

        def pass_on(self, du):
            for i in self.arrays:
                for p in (0, 1):
                    for sign, dv in ((1, 1), (-1, 3)):
                        self.arrived(p, i, du, dv)
                        self.along_v(p, i, du, dv, sign, 0 if sign == 1 else 1)

        def step_one(self):
            for i in self.arrays:
                for p in (0, 1):
                    for du, sign in ((1, 1), (3, -1)):
                        self.arrived(p, i, du, 0)
                        self.along_u(p, i, du, sign, 0 if sign == 1 else 1)
                        for way in (1, -1):
                            self.along_v(p, i, du, 0, way)
                for sign in (1, -1):
                    self.arrived_z(i, sign, 1, 0)
            self.pass_on(0)
            self.step_z(1, 1)

        def step_two(self):
            for i in self.arrays:
                for p in (0, 1):
                    self.arrived(p, i, 2, 0)
                    for way in (1, -1):
                        self.along_v(p, i, 2, 0, way)
            self.step_z(2, 0)
            self.pass_on(1)
            self.step_z(2, 1)
            self.pass_on(3)

        def step_three(self):
            self.step_z(3, 0)
            self.pass_on(2)
            self.step_z(3, 1)

        def finish_z(self):
            for i in self.arrays:
                self.arrived_z(i, 1, 4, 0)
                self.arrived_z(i, -1, 4, 1)

        def finish(self):
            wait_for(self.row.at[pl.ds(0, 4)], self.last_in)

        def totals(self):
            return self.row.at[pl.ds(0, 15)], self.col.at[pl.ds(0, 15)]

    def trace_over(step, axis, here, count):
        mine = traces.at[step * NZ + here]
        for d in range(1, count):
            send(4, mine, mine, trace_in.at[step], **{axis: lax.rem(here + d, count)})

    def trace_total(step, count):
        wait_for(traces.at[pl.ds(step * NZ, count - 1)], trace_in.at[step])
        total = traces[step * NZ]
        for n in range(1, count):
            total = total + traces[step * NZ + n]
        return total

    def halo_begin(stage, state):
        turned = jnp.transpose(state)
        hs[stage, 0] = turned[:OMAX, :].astype(BF16)
        hs[stage, 1] = turned[WIDTH - OMAX :, :].astype(BF16)
        xe[stage, OMAX : OMAX + HEIGHT, 0:WIDTH] = state.astype(BF16)
        hr[stage, 2 * OMAX :, :] = jnp.zeros((WIDTH - 2 * OMAX, HEIGHT), BF16)
        for side, step in ((0, BLOCKS - 1), (1, 1)):
            to = lax.rem(cb + step, BLOCKS)
            send(
                5, hs.at[stage, side], hr.at[stage, pl.ds(side * OMAX, OMAX), :],
                halo_in.at[stage, 0],
                x=to // 8, y=lax.rem(to // 2, NY), c=lax.rem(to, NC),
            )

    def halo_rows(stage):
        wait_for(hs.at[stage], halo_in.at[stage, 0])
        xe[stage, OMAX : OMAX + HEIGHT, WIDTH:] = jnp.transpose(hr[stage].astype(F32)).astype(BF16)
        send(
            6, xe.at[stage, pl.ds(OMAX, OMAX), :], xe.at[stage, pl.ds(OMAX + HEIGHT, OMAX), :],
            halo_in.at[stage, 1], z=near["z", -1],
        )
        send(
            6, xe.at[stage, pl.ds(HEIGHT, OMAX), :], xe.at[stage, pl.ds(0, OMAX), :],
            halo_in.at[stage, 1], z=near["z", 1],
        )

    def halo_end(stage):
        wait_for(xe.at[stage, pl.ds(0, 2 * OMAX), :], halo_in.at[stage, 1])

    def coefficients():
        count = active[0]
        slot = iota((SLOTS, WIDTH), 0)
        shift = jnp.zeros((SLOTS, WIDTH), jnp.int32)
        for k in range(SLOTS):
            shift = jnp.where(slot == k, offsets[k], shift)

        def strengths(block):
            at = jnp.minimum(jnp.maximum(block, 0), BLOCKS - 1)
            values = amp[:, pl.ds(pl.multiple_of(at * WIDTH, WIDTH), WIDTH)]
            level = block * WIDTH + iota((SLOTS, WIDTH), 1)
            inside = (level >= 0) & (level < LEVELS) & (level + shift >= 0)
            inside = inside & (level + shift < LEVELS) & (slot < count)
            return jnp.where(inside, values, 0.0)

        blocks = [cb] + [4 * z + r for r in range(4)]
        squares = []
        own = []
        for block in blocks:
            window = [strengths(block + d) for d in (-1, 0, 1)]
            own.append(window[1])
            squares.append(jnp.concatenate([w * w for w in window], axis=1))
        squares = jnp.concatenate(squares + [jnp.zeros_like(squares[0])] * 3, axis=0)
        high = squares.astype(BF16)
        rest = squares - high.astype(F32)
        mid = rest.astype(BF16)
        low = (rest - mid.astype(F32)).astype(BF16)
        parts = jnp.concatenate([high, mid, low], axis=0)
        which = lax.rem(iota(parts.shape, 0), SLOTS)
        total = jnp.zeros((parts.shape[0], WIDTH), F32)
        source = iota((3 * WIDTH, WIDTH), 0)
        target = iota((3 * WIDTH, WIDTH), 1)
        for k in range(SLOTS):
            pick = jnp.where(source == target + (WIDTH - offsets[k]), 1.0, 0.0).astype(BF16)
            chosen = jnp.where(which == k, parts.astype(F32), 0.0).astype(BF16)
            total = total + jnp.dot(chosen, pick, preferred_element_type=F32)
        total = total[0:64] + total[64:128] + total[128:192]
        outflow = [jnp.sum(total[8 * n : 8 * n + 8], axis=0, keepdims=True) for n in range(5)]
        coef[0, 0:SLOTS, :] = own[0]
        coef[0, SLOTS : 2 * SLOTS, :] = jnp.broadcast_to(outflow[0], (SLOTS, WIDTH))
        for r in range(4):
            table = jnp.concatenate(
                [
                    own[1 + r],
                    jnp.broadcast_to(outflow[1 + r], (SLOTS, WIDTH)),
                    jnp.zeros((WIDTH - 2 * SLOTS, WIDTH), F32),
                ],
                axis=0,
            )
            coef[1 + r] = jnp.transpose(table)
        source = iota((2 * WIDTH, WIDTH), 0)
        target = iota((2 * WIDTH, WIDTH), 1)
        for k in range(SLOTS):
            at = target + offsets[k]
            at = jnp.where(at < 0, at + (WIDTH + 2 * OMAX), at)
            onehot[:, k * WIDTH : (k + 1) * WIDTH] = jnp.where(source == at, 1.0, 0.0).astype(BF16)

    def dissipator(stage, state):
        shifted[...] = jnp.dot(xe[stage], onehot[...], preferred_element_type=F32)
        for r in range(4):
            rows = slice(r * WIDTH, (r + 1) * WIDTH)
            by_row = coef[1 + r]
            flow = by_row[:, SLOTS : SLOTS + 1] + coef[0, SLOTS : SLOTS + 1, :]
            total = -0.5 * flow * state[rows, :]
            for k in range(SLOTS):
                span = WIDTH + 2 * OMAX
                moved = shifted[r * WIDTH : r * WIDTH + span, k * WIDTH : (k + 1) * WIDTH]
                moved = pltpu.roll(moved, lax.rem(span - OMAX - offsets[k], span), 0)[0:WIDTH]
                total = total + by_row[:, k : k + 1] * coef[0, k : k + 1, :] * moved
            diss[rows, :] = total

    def commutator(stage, late):
        lefts, rights = [], []
        for dx in range(NX):
            for dy in range(NY):
                if (dx == 2 or dy == 2 or (dx, dy) == (3, 3)) != late:
                    continue
                xk, yk = lax.rem(x + NX - dx, NX), lax.rem(y + NY - dy, NY)
                owner = NC * (2 * xk + yk // 2)
                slot = 4 * dx + dy
                rows = pl.ds(pl.multiple_of(lax.rem(yk, 2) * WIDTH, WIDTH), WIDTH)
                lefts.append(row1[slot, 1] if stage == 0 else row2[slot, 0])
                lefts.append(row1[slot, 0])
                upper = [col1[owner + i, 0, rows, :] for i in range(NC)]
                if stage == 0:
                    lower = [col1[owner + i, 1, rows, :] for i in range(NC)]
                else:
                    lower = [col2[owner + i, 0, rows, :] for i in range(NC)]
                rights.append(jnp.concatenate(upper, axis=1))
                rights.append(jnp.concatenate(lower, axis=1))
        product = jnp.dot(
            jnp.concatenate(lefts, axis=1),
            jnp.concatenate(rights, axis=0),
            preferred_element_type=F32,
        )
        for i in range(NC):
            mine = product[:, i * WIDTH : (i + 1) * WIDTH]
            if late:
                acc[stage, i] += mine
            else:
                acc[stage, i] = mine

    def joined(stage):
        send(7, acc.at[stage, other], peer.at[stage], peer_in.at[stage], c=other)
        wait_for(peer.at[stage], peer_in.at[stage])
        return acc[stage, c] + peer[stage]

    def spread_begin(n, value):
        ts[n] = value.astype(BF16)
        for d in range(1, NX):
            to = lax.rem(x + d, NX)
            send(
                8, ts.at[n, pl.ds(pl.multiple_of(to * WIDTH, WIDTH), WIDTH), :],
                tr.at[4 * n + x], spread_in.at[n, d - 1], x=to,
            )
        tr[4 * n + x] = ts[n, pl.ds(pl.multiple_of(x * WIDTH, WIDTH), WIDTH), :]

    def turn_copy(n, s):
        return pltpu.make_async_remote_copy(
            src_ref=tr.at[4 * n + s],
            dst_ref=tx.at[n, lax.rem(cb, 4)],
            send_sem=turn_in.at[n, 0, s],
            recv_sem=turn_in.at[n, 1, lax.rem(cb, 4)],
            device_id=dict(
                z=2 * s + y // 2, x=z // 2, y=2 * lax.rem(z, 2) + x // 2, c=lax.rem(x, 2)
            ),
            device_id_type=MESH,
        )

    def turn_stays(s):
        there = (2 * s + y // 2 == z) & (z // 2 == x)
        return there & (2 * lax.rem(z, 2) + x // 2 == y) & (lax.rem(x, 2) == c)

    def turn_begin(n):
        for d in (0, 1, 3, 2):
            s = lax.rem(x + NX - d, NX)
            if d:
                wait_for(tr.at[4 * n + s], spread_in.at[n, d - 1])

            def go(s=s):
                turn_copy(n, s).start()

            def keep(s=s):
                tx[n, lax.rem(cb, 4)] = tr[4 * n + s]

            pl.when(jnp.logical_not(turn_stays(s)))(go)
            pl.when(turn_stays(s))(keep)

    def turn_sent(n):
        for s in range(NX):

            def left(s=s):
                turn_copy(n, s).wait_send()

            pl.when(jnp.logical_not(turn_stays(s)))(left)

    def turn_arrived(n, q):
        own = (cb // 4 == z) & (2 * lax.rem(z, 2) + q // 2 == y) & (q % 2 == c)
        own = own & (lax.rem(cb, 4) == x)
        pl.when(jnp.logical_not(own))(lambda: wait_for(tx.at[n, q], turn_in.at[n, 1, q]))

    first = Gather(0, row1, rows1_in, last_in.at[0], col1, cols1_in, part1, part_in.at[0])
    for load in loads[:3]:
        load.wait()
    row1[0, 0] = ham[...]
    row1[0, 1] = (real[...] + imag[...]).astype(BF16)
    for i in range(2):
        rows = slice(i * WIDTH, (i + 1) * WIDTH)
        part1[0, rows, :] = quarter(ham, 2 * i + other)
        part1[1, rows, :] = -quarter(row1.at[0, 1], 2 * i + other)
        col1[z * NC + c, 0, rows, :] = quarter(ham, 2 * i + c)
        col1[z * NC + c, 1, rows, :] = -quarter(row1.at[0, 1], 2 * i + c)
    on_diagonal = iota((HEIGHT, WIDTH), 0) + z * HEIGHT == iota((HEIGHT, WIDTH), 1) + cb * WIDTH
    diagonal = jnp.sum(jnp.where(on_diagonal, real[...], 0.0), axis=0, keepdims=True)
    diagonal = jnp.sum(diagonal, axis=1, keepdims=True)
    traces[x] = jnp.broadcast_to(diagonal, (8, WIDTH))
    pl.semaphore_wait(barrier, len(greeted))
    first.begin()
    halo_begin(0, real[...] - imag[...])
    first.step_one()
    halo_rows(0)
    for load in loads[3:]:
        load.wait()
    coefficients()
    first.step_two()
    trace_over(0, "x", x, NX)
    halo_end(0)
    dissipator(0, real[...] - imag[...])
    first.step_three()
    traces[NZ + y] = trace_total(0, NX)
    trace_over(1, "y", y, NY)
    first.finish_z()
    commutator(0, False)
    traces[2 * NZ + c] = trace_total(1, NY)
    trace_over(2, "c", c, NC)
    first.finish()
    commutator(0, True)
    traces[3 * NZ + z] = trace_total(2, NC)
    trace_over(3, "z", z, NZ)
    drift1[...] = diss[...] - joined(0)
    middle[...] = real[...] - imag[...] + STEP * drift1[...]

    second = Gather(2, row2, rows2_in, last_in.at[1], col2, cols2_in, part2, part_in.at[1])
    row2[0, 0] = middle[...].astype(BF16)
    for i in range(2):
        rows = slice(i * WIDTH, (i + 1) * WIDTH)
        part2[0, rows, :] = -quarter(row2.at[0, 0], 2 * i + other)
        col2[z * NC + c, 0, rows, :] = -quarter(row2.at[0, 0], 2 * i + c)
    second.begin()
    halo_begin(1, middle[...])
    second.step_one()
    halo_rows(1)
    second.step_two()
    halo_end(1)
    dissipator(1, middle[...])
    rescale = LEVELS / trace_total(3, NZ)
    factor[...] = rescale
    rescale = jnp.concatenate([rescale] * (HEIGHT // 8), axis=0)
    drift1[...] = drift1[...] + rescale * diss[...]
    spread_begin(0, drift1[...])
    second.step_three()
    second.finish_z()
    commutator(1, False)
    turn_begin(0)
    second.finish()
    commutator(1, True)
    middle[...] = rescale * joined(1)
    spread_begin(1, middle[...])
    turn_begin(1)
    weight = 0.25 * STEP
    for q in range(4):
        rows = slice(q * WIDTH, (q + 1) * WIDTH)
        turn_arrived(0, q)
        there = jnp.transpose(tx[0, q].astype(F32))
        out_real[rows, :] = real[rows, :] + weight * (drift1[rows, :] + there + middle[rows, :])
        out_imag[rows, :] = imag[rows, :] + weight * (there - drift1[rows, :] + middle[rows, :])
    pltpu.make_async_copy(factor, next_factor, stored.at[2]).start()
    for q in range(4):
        rows = slice(q * WIDTH, (q + 1) * WIDTH)
        turn_arrived(1, q)
        there = weight * jnp.transpose(tx[1, q].astype(F32))
        out_real[rows, :] = out_real[rows, :] + there
        out_imag[rows, :] = out_imag[rows, :] - there
        for n, (out, to) in enumerate(((out_real, next_real), (out_imag, next_imag))):
            pltpu.make_async_copy(out.at[rows, :], to.at[rows, :], stored.at[n]).start()
    turn_sent(0)
    turn_sent(1)
    send.drain(
        *first.totals(), *second.totals(), traces.at[pl.ds(0, 14)], hs,
        xe.at[0, pl.ds(0, 4 * OMAX), :], peer, tr.at[pl.ds(0, 6)],
    )
    wait_for(factor, stored.at[2])
    wait_for(out_real, stored.at[0])
    wait_for(out_imag, stored.at[1])


def local(real, imag, ham, amp, offsets, active):
    hbm = pl.BlockSpec(memory_space=pltpu.HBM)
    dma = pltpu.SemaphoreType.DMA
    block = jax.ShapeDtypeStruct((HEIGHT, WIDTH), F32)
    next_real, next_imag, factor = pl.pallas_call(
        kernel,
        out_shape=(block, block, jax.ShapeDtypeStruct((8, WIDTH), F32)),
        in_specs=[hbm] * 6,
        out_specs=(hbm, hbm, hbm),
        scratch_shapes=[
            pltpu.VMEM((HEIGHT, WIDTH), F32),
            pltpu.VMEM((HEIGHT, WIDTH), F32),
            pltpu.VMEM((HEIGHT, WIDTH), BF16),
            pltpu.VMEM((SLOTS, LEVELS), F32),
            pltpu.SMEM((SLOTS,), jnp.int32),
            pltpu.SMEM((1,), jnp.int32),
            dma((6,)),
            pltpu.VMEM((HEIGHT, WIDTH), F32),
            pltpu.VMEM((HEIGHT, WIDTH), F32),
            pltpu.VMEM((8, WIDTH), F32),
            dma((3,)),
            pltpu.VMEM((NX * NY, 2, HEIGHT, WIDTH), BF16),
            pltpu.VMEM((NX * NY, 1, HEIGHT, WIDTH), BF16),
            pltpu.VMEM((NZ * NC, 2, 2 * WIDTH, WIDTH), BF16),
            pltpu.VMEM((NZ * NC, 1, 2 * WIDTH, WIDTH), BF16),
            pltpu.VMEM((2, 2 * WIDTH, WIDTH), BF16),
            pltpu.VMEM((1, 2 * WIDTH, WIDTH), BF16),
            pltpu.VMEM((2, NC, HEIGHT, WIDTH), F32),
            pltpu.VMEM((2, HEIGHT, WIDTH), F32),
            pltpu.VMEM((4 * NZ, 8, WIDTH), F32),
            pltpu.VMEM((2, 2, OMAX, HEIGHT), BF16),
            pltpu.VMEM((2, WIDTH, HEIGHT), BF16),
            pltpu.VMEM((2, HEIGHT + 2 * OMAX, 2 * WIDTH), BF16),
            pltpu.VMEM((HEIGHT + 2 * OMAX, SLOTS * WIDTH), F32),
            pltpu.VMEM((2 * WIDTH, SLOTS * WIDTH), BF16),
            pltpu.VMEM((5, WIDTH, WIDTH), F32),
            pltpu.VMEM((HEIGHT, WIDTH), F32),
            pltpu.VMEM((HEIGHT, WIDTH), F32),
            pltpu.VMEM((HEIGHT, WIDTH), F32),
            pltpu.VMEM((2, HEIGHT, WIDTH), BF16),
            pltpu.VMEM((8, WIDTH, WIDTH), BF16),
            pltpu.VMEM((2, 4, WIDTH, WIDTH), BF16),
            dma((9,)),
            dma((2, 2, 11)),
            dma((1, 2, 11)),
            dma((2,)),
            dma((2, 2, 7)),
            dma((1, 2, 7)),
            dma((2,)),
            dma((2,)),
            dma((4,)),
            dma((2, 2)),
            dma((2, 3)),
            dma((2, 2, 4)),
        ],
        compiler_params=pltpu.CompilerParams(
            has_side_effects=True, collective_id=0, vmem_limit_bytes=63 * 1024 * 1024
        ),
    )(real, imag, ham, amp, offsets, active)
    return next_real * factor[0, 0], next_imag * factor[0, 0]


def solution(mesh):
    split = Mesh(mesh.devices.reshape(NZ, NX, NY, NC), ("z", "x", "y", "c"))
    tiled = P("z", ("x", "y", "c"))
    return jax.shard_map(
        local,
        mesh=split,
        in_specs=(tiled, tiled, tiled, P(), P(), P()),
        out_specs=(tiled, tiled),
        check_vma=False,
    )
```
